32 devices in a mesh: rows: 16 (over z, x, core), chan: 2 (over y).
Axes of the slice: x: 2, y: 2, z: 4, core: 2. Of those that a mesh axis runs over, the one named last changes fastest.
Arguments:
- pixels: float32 [1024, 16384], P(('chan', 'rows')), parts along dimension 0, may hold values from -6 to 6
- row_taps: float32 [32768], P(('chan', 'rows')), parts along dimension 0, may hold values from -0.046875 to 0.046875
- column_taps: float32 [1024], P(('chan', 'rows')), parts along dimension 0, may hold values from -0.25 to 0.25
- stencil: float32 [6, 3], P('chan'), parts along dimension 0, may hold values from -3 to 3
Outputs:
- filtered: float32 [1024, 16384], P(('chan', 'rows')), parts along dimension 0
The draws below stay inside these ranges and needn't reach their ends.
There are 2 independent parts, one for each index of `chan`. The reference program is written for one: setup_inputs(seed, part) draws one part's arguments, and reference() takes and returns one part's arrays. A program takes and returns all parts, laid end to end along the dimension named above; each array names one. Nothing has to cross between parts.
All inputs are finite; a program needn't handle non-finite values.
Results may differ from the reference program's by a relative error of at most 0.0003.
Values sent between devices are 32-bit elements; how exact they have to be, the bound alone decides.
A program may use at most 128 MiB of HBM per device.

```python
import jax
import jax.numpy as jnp

NX = 16384
NY = 512


def steps_of(key, dims, shards, least, largest):
    def one(position, parts):
        heights = jax.random.uniform(jax.random.fold_in(jax.random.fold_in(key, 6), position), (parts,), jnp.float32, least / len(shards), largest / len(shards))
        return jnp.repeat(jnp.exp(heights), dims[position] // parts).reshape((-1,) + (1,) * (len(dims) - position - 1))

    loudness = one(*shards[0])
    for cut in shards[1:]:
        loudness = loudness * one(*cut)
    return loudness


def bell_draw(key, dims, scale, limit, pieces=(), kind=jnp.bfloat16):
    loudness = steps_of(key, dims, pieces, -0.22, 0.18) if pieces else 1.0
    values = jax.random.normal(key, dims, jnp.float32) * scale * loudness
    return jnp.minimum(jnp.maximum(values, -limit), limit).astype(kind)


def setup_inputs(seed: int = 0, part: int = 0) -> dict:
    streams_of = jax.random.split(jax.random.key(seed), 5)
    part_keys = jax.random.split(jax.random.fold_in(streams_of[4], part), 5)
    return {
        "pixels": bell_draw(part_keys[0], (NY, NX), 1.0, 6.0, ((0, 16),), jnp.float32),
        "row_taps": bell_draw(part_keys[1], (NX,), NX ** -0.5, 0.046875, ((0, 16),), jnp.float32),
        "column_taps": bell_draw(part_keys[2], (NY,), NY ** -0.5, 0.25, ((0, 16),), jnp.float32),
        "stencil": bell_draw(part_keys[3], (3, 3), 0.5, 3.0, (), jnp.float32),
    }


def reference(pixels, row_taps, column_taps, stencil):
    row_spectrum = jnp.fft.rfft(row_taps)
    column_spectrum = jnp.fft.rfft(column_taps)
    row_done = jnp.fft.irfft(jnp.fft.rfft(pixels, axis=1) * row_spectrum[None, :], n=NX, axis=1)
    combined = jnp.fft.irfft(jnp.fft.rfft(row_done, axis=0) * column_spectrum[:, None], n=NY, axis=0)
    filtered = combined.astype(pixels.dtype)
    for offset_row in range(3):
        for offset_col in range(3):
            moved = jnp.roll(pixels, (1 - offset_row, 1 - offset_col), axis=(0, 1))
            filtered = filtered + stencil[offset_row, offset_col] * moved
    return filtered
```

```python
import functools
import math

import jax
import jax.numpy as jnp
import numpy as np
from jax import lax
from jax.experimental import pallas as pl
from jax.experimental.pallas import tpu as pltpu
from jax.sharding import PartitionSpec as P

dft_precision = lax.Precision.HIGH
row_forms = ("kj,rjm->rkm", "rkm,ml->rkl")
column_forms = ("kj,jmc->kmc", "kmc,ml->klc")


def padded_2(cells, sides, width):
    for axis, dim in sides:
        count = lax.axis_size(axis)
        head = lax.slice_in_dim(cells, 0, width, axis=dim)
        tail = lax.slice_in_dim(cells, cells.shape[dim] - width, cells.shape[dim], axis=dim)
        cells = jnp.concatenate(
            [
                lax.ppermute(tail, axis, [(i, (i + 1) % count) for i in range(count)]),
                cells,
                lax.ppermute(head, axis, [((i + 1) % count, i) for i in range(count)]),
            ],
            axis=dim,
        )
    return cells


def split_length(length):
    factor = int(math.isqrt(length))
    while length % factor:
        factor -= 1
    return (length // factor, factor)


def dft_tables(length):
    positions = jnp.arange(length, dtype=jnp.int32)
    product = positions[:, None] * positions[None, :] % length
    angles = product.astype(jnp.float32) * (2.0 * math.pi / length)
    return (jnp.cos(angles), -jnp.sin(angles))


def prepare(length, twist_shape):
    outer_len, inner_len = split_length(length)
    cos_outer, sin_outer = dft_tables(outer_len)
    cos_inner, sin_inner = dft_tables(inner_len)
    outer_pos = jnp.arange(outer_len, dtype=jnp.int32)
    inner_pos = jnp.arange(inner_len, dtype=jnp.int32)
    product = outer_pos[:, None] * inner_pos[None, :] % length
    angles = product.astype(jnp.float32) * (2.0 * math.pi / length)
    twist_real = jnp.cos(angles).reshape(twist_shape)
    twist_imag = (-jnp.sin(angles)).reshape(twist_shape)
    return (
        outer_len,
        inner_len,
        cos_outer,
        sin_outer,
        cos_inner,
        sin_inner,
        twist_real,
        twist_imag,
    )


def contract(form, left, right):
    return jnp.einsum(
        form, left, right, precision=dft_precision, preferred_element_type=jnp.float32
    )


def forward(values, tables, forms):
    outer_len, inner_len, cos_outer, sin_outer, cos_inner, sin_inner, twist_real, twist_imag = (
        tables
    )
    first_real = contract(forms[0], cos_outer, values)
    first_imag = contract(forms[0], sin_outer, values)
    turned_real = first_real * twist_real - first_imag * twist_imag
    turned_imag = first_real * twist_imag + first_imag * twist_real
    out_real = contract(forms[1], turned_real, cos_inner) - contract(
        forms[1], turned_imag, sin_inner
    )
    out_imag = contract(forms[1], turned_real, sin_inner) + contract(
        forms[1], turned_imag, cos_inner
    )
    return (out_real, out_imag)


def inverse(spec_real, spec_imag, tables, forms):
    outer_len, inner_len, cos_outer, sin_outer, cos_inner, sin_inner, twist_real, twist_imag = (
        tables
    )
    back_real = contract(forms[1], spec_real, cos_inner) + contract(forms[1], spec_imag, sin_inner)
    back_imag = contract(forms[1], spec_imag, cos_inner) - contract(forms[1], spec_real, sin_inner)
    turned_real = back_real * twist_real + back_imag * twist_imag
    turned_imag = back_imag * twist_real - back_real * twist_imag
    result = contract(forms[0], cos_outer, turned_real) + contract(forms[0], sin_outer, turned_imag)
    return result / float(outer_len * inner_len)


def convolve(values, filter_spec, tables, forms):
    spec_real, spec_imag = forward(values, tables, forms)
    filter_real, filter_imag = filter_spec
    prod_real = spec_real * filter_real - spec_imag * filter_imag
    prod_imag = spec_real * filter_imag + spec_imag * filter_real
    return inverse(prod_real, prod_imag, tables, forms)


def body(pixels, row_taps, column_taps, stencil):
    rows_dev, row_length = pixels.shape
    devices_rows = lax.axis_size("rows")
    whole_row, whole_column = (
        lax.all_gather(row_taps, "rows", axis=0, tiled=True),
        lax.all_gather(column_taps, "rows", axis=0, tiled=True),
    )
    column_length = whole_column.shape[0]
    row_tables = prepare(row_length, (1, split_length(row_length)[0], split_length(row_length)[1]))
    column_tables = prepare(
        column_length, (split_length(column_length)[0], split_length(column_length)[1], 1)
    )
    row_filter = forward(whole_row.reshape(1, row_tables[0], row_tables[1]), row_tables, row_forms)
    column_filter = forward(
        whole_column.reshape(column_tables[0], column_tables[1], 1), column_tables, column_forms
    )
    cols_dev = row_length // devices_rows
    lane_width = min(128, cols_dev)
    groups = cols_dev // lane_width
    padded = padded_2(pixels, (("rows", 0),), 1)
    shaped = pixels.reshape(pixels.shape[0], row_tables[0], row_tables[1])
    blocks = (
        convolve(shaped, row_filter, row_tables, row_forms)
        .reshape(pixels.shape)
        .reshape(rows_dev, groups, devices_rows * lane_width)
    )
    moved = lax.all_to_all(blocks, "rows", split_axis=2, concat_axis=0, tiled=True)
    shaped = moved.reshape(column_tables[0], column_tables[1], -1)
    result = lax.all_to_all(
        convolve(shaped, column_filter, column_tables, column_forms).reshape(moved.shape),
        "rows",
        split_axis=0,
        concat_axis=2,
        tiled=True,
    )
    convolved = result.reshape(rows_dev, row_length)
    filtered = convolved
    for offset_row in range(3):
        row_band = padded[offset_row : offset_row + rows_dev]
        for offset_col in range(3):
            filtered = filtered + stencil[offset_row, offset_col] * jnp.roll(
                row_band, 1 - offset_col, axis=1
            )
    return filtered


def split_bf16(values):
    high = values.astype(jnp.bfloat16)
    low = (values - high.astype(jnp.float32)).astype(jnp.bfloat16)
    return high, low


def mm(left, right):
    return jnp.dot(left, right, preferred_element_type=jnp.float32)


def mm3(left, right):
    return mm(left[0], right[0]) + (mm(left[0], right[1]) + mm(left[1], right[0]))


def host_tables(side):
    length = side * side
    index = np.arange(side)
    product = index[:, None] * index[None, :]
    angle = 2.0 * np.pi * (product % side) / side
    cos, sin = np.cos(angle), np.sin(angle)
    table = np.block([[cos, sin], [-sin, cos]]).astype(np.float32)

    def halves(array):
        high = array.astype(jnp.bfloat16)
        low = (array - high.astype(np.float32)).astype(jnp.bfloat16)
        return high, low

    fwd_high, fwd_low = halves(table)
    inv_high, inv_low = halves(np.ascontiguousarray(table.T))
    turn = 2.0 * np.pi * product / length
    return (
        fwd_high,
        fwd_low,
        inv_high,
        inv_low,
        np.cos(turn).astype(np.float32),
        (-np.sin(turn)).astype(np.float32),
    )


def kernel(
    dims,
    pixels,
    top_row,
    bottom_row,
    taps,
    stencil,
    fwd_high,
    fwd_low,
    inv_high,
    inv_low,
    twist_real,
    twist_imag,
    out,
    recv,
    recv_high,
    recv_low,
    ready,
    back,
    padded,
    halo_above,
    halo_below,
    all_taps,
    circ_high,
    circ_low,
    filter_real,
    filter_imag,
    send_px,
    recv_px,
    send_tap,
    recv_tap,
    send_halo,
    recv_halo,
    send_back,
    recv_back,
    local_sem,
):
    count, rows_dev, side = dims
    groups = rows_dev // 8
    cols_dev = side * side // count
    a_dev = cols_dev // 128
    column_length = count * rows_dev
    tap_rows = taps.shape[0]
    row_tap_rows = a_dev
    me = lax.axis_index("rows")

    def peer(step):
        return lax.rem(me + step, count)

    def source(step):
        return lax.rem(me + count - step, count)

    barrier = pltpu.get_barrier_semaphore()

    @pl.loop(1, count)
    def _(step):
        pl.semaphore_signal(barrier, inc=1, device_id={"rows": peer(step)})

    pl.semaphore_wait(barrier, count - 1)

    def px_copy(step):
        to = peer(step)
        return pltpu.make_async_remote_copy(
            src_ref=pixels.at[:, pl.ds(pl.multiple_of(to * cols_dev, 128), cols_dev)],
            dst_ref=recv.at[pl.ds(pl.multiple_of(me * rows_dev, 8), rows_dev), :],
            send_sem=send_px.at[step],
            recv_sem=recv_px.at[step],
            device_id={"rows": to},
        )

    def tap_copy(step):
        return pltpu.make_async_remote_copy(
            src_ref=taps,
            dst_ref=all_taps.at[me],
            send_sem=send_tap.at[step],
            recv_sem=recv_tap.at[step],
            device_id={"rows": peer(step)},
        )

    def halo_copy(which):
        return pltpu.make_async_remote_copy(
            src_ref=(bottom_row, top_row)[which],
            dst_ref=(halo_above, halo_below)[which],
            send_sem=send_halo.at[which],
            recv_sem=recv_halo.at[which],
            device_id={"rows": peer(1 if which == 0 else count - 1)},
        )

    @pl.loop(1, count)
    def _(step):
        tap_copy(step).start()

    halo_copy(0).start()
    halo_copy(1).start()

    @pl.loop(1, count)
    def _(step):
        px_copy(step).start()

    own_px = pltpu.make_async_copy(
        pixels.at[:, pl.ds(pl.multiple_of(me * cols_dev, 128), cols_dev)],
        recv.at[pl.ds(pl.multiple_of(me * rows_dev, 8), rows_dev), :],
        local_sem.at[0],
    )
    own_px.start()
    own_tap = pltpu.make_async_copy(taps, all_taps.at[me], local_sem.at[1])
    own_tap.start()

    padded[8 : 8 + rows_dev, :] = pixels[...]
    halo_copy(0).wait_recv()
    halo_copy(1).wait_recv()
    padded[7:8, :] = halo_above[...]
    padded[8 + rows_dev : 9 + rows_dev, :] = halo_below[...]
    width = side * side
    for group in range(groups):
        base = group * 8
        above = padded[7 + base : 15 + base, :]
        here = padded[8 + base : 16 + base, :]
        below = padded[9 + base : 17 + base, :]
        sums = [
            stencil[0, b] * above + stencil[1, b] * here + stencil[2, b] * below for b in range(3)
        ]
        out[base : base + 8, :] = (
            sums[1] + pltpu.roll(sums[0], 1, 1) + pltpu.roll(sums[2], width - 1, 1)
        )

    own_tap.wait()

    @pl.loop(1, count)
    def _(step):
        tap_copy(step).wait_recv()

    tap_sum = all_taps[0, row_tap_rows:tap_rows, :]
    for rank in range(1, count):
        tap_sum = tap_sum + all_taps[rank, row_tap_rows:tap_rows, :]
    line = jnp.concatenate(
        [tap_sum[j : j + 1, :] for j in range(column_length // 128)], axis=1
    )
    per_block = 128 // rows_dev
    line = jnp.broadcast_to(line, (128, column_length))
    turned = [
        pltpu.roll(line, block * 128, 1, stride=1, stride_axis=0)
        for block in range(column_length // 128)
    ]
    for group in range(groups):
        part = jnp.concatenate(
            [
                turned[rank // per_block][
                    (rank % per_block) * rows_dev + group * 8 :
                    (rank % per_block) * rows_dev + group * 8 + 8
                ]
                for rank in range(count)
            ],
            axis=0,
        )
        high, low = split_bf16(part)
        circ_high[group] = high
        circ_low[group] = low

    forward_table = (fwd_high, fwd_low)
    inverse_table = (inv_high, inv_low)

    def loaded(table):
        return (table[0][...], table[1][...])

    def swap(real, imag):
        return jnp.concatenate(
            [
                jnp.concatenate([real[:, :side], imag[:, :side]], axis=1),
                jnp.concatenate([real[:, side:], imag[:, side:]], axis=1),
            ],
            axis=0,
        )

    def spectrum(cells):
        first = mm3(loaded(forward_table), split_bf16(cells))
        real, imag = first[:side], first[side:]
        turn_r = jnp.concatenate([twist_real[...]] * 2, axis=1)
        turn_i = jnp.concatenate([twist_imag[...]] * 2, axis=1)
        turned_cells = swap(real * turn_r - imag * turn_i, real * turn_i + imag * turn_r)
        return mm3(split_bf16(turned_cells), loaded(inverse_table))

    def inverse_of(real, imag):
        cells = jnp.concatenate([real, imag], axis=1)
        first = mm3(split_bf16(cells), loaded(forward_table))
        real, imag = first[:, :side], first[:, side:]
        turn_r = jnp.concatenate([twist_real[...]] * 2, axis=0)
        turn_i = jnp.concatenate([twist_imag[...]] * 2, axis=0)
        back_real = real * turn_r + imag * turn_i
        back_imag = imag * turn_r - real * turn_i
        cells = jnp.concatenate(
            [
                jnp.concatenate([back_real[:side], back_real[side:]], axis=1),
                jnp.concatenate([back_imag[:side], back_imag[side:]], axis=1),
            ],
            axis=0,
        )
        return mm3(loaded(inverse_table), split_bf16(cells))

    row_filter = jnp.concatenate(
        [all_taps[rank, 0:row_tap_rows, :] for rank in range(count)], axis=0
    )
    nothing = jnp.zeros_like(row_filter)
    filter_spec = spectrum(
        jnp.concatenate(
            [
                jnp.concatenate([row_filter, nothing], axis=1),
                jnp.concatenate([nothing, nothing], axis=1),
            ],
            axis=0,
        )
    )[:side]
    filter_real[...] = filter_spec[:, :side] * (1.0 / (side * side))
    filter_imag[...] = filter_spec[:, side:] * (1.0 / (side * side))

    def take(rank):
        at = pl.ds(pl.multiple_of(rank * rows_dev, 16), rows_dev)
        high, low = split_bf16(recv[at, :])
        recv_high[at, :] = high
        recv_low[at, :] = low

    own_px.wait()
    take(me)

    @pl.loop(1, count)
    def _(step):
        px_copy(step).wait_recv()
        take(source(step))

    flat_ready = ready.reshape(groups * count * 8 * a_dev, 128)

    def back_copy(group, step):
        to = peer(step)
        return pltpu.make_async_remote_copy(
            src_ref=ready.at[pl.ds((group * count + to) * 8, 8)],
            dst_ref=back.at[pl.ds(group * 8, 8), pl.ds(pl.multiple_of(me * a_dev, 8), a_dev), :],
            send_sem=send_back.at[group, step],
            recv_sem=recv_back.at[group, step],
            device_id={"rows": to},
        )

    def own_back(group):
        return pltpu.make_async_copy(
            ready.at[pl.ds((group * count + me) * 8, 8)],
            back.at[pl.ds(group * 8, 8), pl.ds(pl.multiple_of(me * a_dev, 8), a_dev), :],
            local_sem.at[2 + group],
        )

    tile = 256
    for group in range(groups):
        for piece in range(cols_dev // tile):
            cut = slice(piece * tile, (piece + 1) * tile)
            done = mm3(
                (circ_high[group], circ_low[group]), (recv_high[:, cut], recv_low[:, cut])
            )
            for j in range(tile // 128):
                flat_ready[
                    pl.ds(group * count * 8 * a_dev + piece * (tile // 128) + j, count * 8, stride=a_dev), :
                ] = done[:, j * 128 : (j + 1) * 128]

        @pl.loop(1, count)
        def _(step, group=group):
            back_copy(group, step).start()

        own_back(group).start()

    flat_back = back.reshape(rows_dev * side, side)
    for group in range(groups):
        own_back(group).wait()

        @pl.loop(1, count)
        def _(step, group=group):
            back_copy(group, step).wait_recv()

        for half in range(2):
            row = group * 8 + half * 4
            cells = jnp.concatenate(
                [
                    jnp.concatenate([back[row], back[row + 2]], axis=1),
                    jnp.concatenate([back[row + 1], back[row + 3]], axis=1),
                ],
                axis=0,
            )
            spec = spectrum(cells)
            real, imag = spec[:, :side], spec[:, side:]
            filt_r = jnp.concatenate([filter_real[...]] * 2, axis=0)
            filt_i = jnp.concatenate([filter_imag[...]] * 2, axis=0)
            done = inverse_of(real * filt_r - imag * filt_i, real * filt_i + imag * filt_r)
            back[row] = done[:side, :side]
            back[row + 1] = done[side:, :side]
            back[row + 2] = done[:side, side:]
            back[row + 3] = done[side:, side:]
        for a in range(side):
            cut = slice(a * side, (a + 1) * side)
            out[group * 8 : group * 8 + 8, cut] += flat_back[
                pl.ds(group * 8 * side + a, 8, stride=side), :
            ]

    halo_copy(0).wait_send()
    halo_copy(1).wait_send()

    @pl.loop(1, count)
    def _(step):
        tap_copy(step).wait_send()
        px_copy(step).wait_send()
        for group in range(groups):
            back_copy(group, step).wait_send()


def fits(pixels, row_taps, column_taps):
    rows_dev, row_length = pixels.shape
    count = lax.axis_size("rows")
    side = math.isqrt(row_length)
    return (
        side == 128
        and side * side == row_length
        and row_length % (count * 1024) == 0
        and rows_dev % 16 == 0
        and 128 % rows_dev == 0
        and (count * rows_dev) % 128 == 0
    )


def fused(pixels, row_taps, column_taps, stencil):
    rows_dev, row_length = pixels.shape
    count = lax.axis_size("rows")
    side = math.isqrt(row_length)
    column_length = rows_dev * count
    cols_dev = row_length // count
    a_dev = cols_dev // 128
    groups = rows_dev // 8
    me = lax.axis_index("rows")
    slots = -(-column_length // 1024) * 1024
    wanted = (column_length - jnp.arange(slots, dtype=jnp.int32)) % column_length
    wanted = jnp.where(jnp.arange(slots) < column_length, wanted, -1)
    held = me * rows_dev + jnp.arange(rows_dev, dtype=jnp.int32)
    placed = jnp.sum(
        jnp.where(wanted[:, None] == held[None, :], column_taps[None, :], 0.0), axis=1
    )
    taps = jnp.concatenate([row_taps.reshape(a_dev, 128), placed.reshape(slots // 128, 128)])
    tables = [jnp.asarray(table) for table in host_tables(side)]
    vmem = pl.BlockSpec(memory_space=pltpu.VMEM)
    f32, bf16 = jnp.float32, jnp.bfloat16
    dma = pltpu.SemaphoreType.DMA
    return pl.pallas_call(
        functools.partial(kernel, (count, rows_dev, side)),
        out_shape=jax.ShapeDtypeStruct(pixels.shape, f32),
        in_specs=[vmem] * 4 + [pl.BlockSpec(memory_space=pltpu.SMEM)] + [vmem] * 6,
        out_specs=vmem,
        scratch_shapes=[
            pltpu.VMEM((column_length, cols_dev), f32),
            pltpu.VMEM((column_length, cols_dev), bf16),
            pltpu.VMEM((column_length, cols_dev), bf16),
            pltpu.VMEM((column_length, a_dev, 128), f32),
            pltpu.VMEM((rows_dev, side, side), f32),
            pltpu.VMEM((rows_dev + 16, row_length), f32),
            pltpu.VMEM((1, row_length), f32),
            pltpu.VMEM((1, row_length), f32),
            pltpu.VMEM((count,) + taps.shape, f32),
            pltpu.VMEM((groups, count * 8, column_length), bf16),
            pltpu.VMEM((groups, count * 8, column_length), bf16),
            pltpu.VMEM((side, side), f32),
            pltpu.VMEM((side, side), f32),
            dma((count,)),
            dma((count,)),
            dma((count,)),
            dma((count,)),
            dma((2,)),
            dma((2,)),
            dma((groups, count)),
            dma((groups, count)),
            dma((2 + groups,)),
        ],
        compiler_params=pltpu.CompilerParams(
            collective_id=0, has_side_effects=True, vmem_limit_bytes=48 * 1024 * 1024
        ),
    )(pixels, pixels[:1], pixels[rows_dev - 1 :], taps, stencil, *tables)


def chosen(pixels, row_taps, column_taps, stencil):
    if fits(pixels, row_taps, column_taps):
        return fused(pixels, row_taps, column_taps, stencil)
    return body(pixels, row_taps, column_taps, stencil)


def solution(mesh):
    in_specs = (
        P(("chan", "rows"), None),
        P(("chan", "rows")),
        P(("chan", "rows")),
        P("chan", None),
    )
    out_specs = P(("chan", "rows"), None)
    return jax.shard_map(chosen, mesh=mesh, in_specs=in_specs, out_specs=out_specs, check_vma=False)
```

```python
import functools
import math

import jax
import jax.numpy as jnp
import numpy as np
from jax import lax
from jax.experimental import pallas as pl
from jax.experimental.pallas import tpu as pltpu
from jax.sharding import PartitionSpec as P

dft_precision = lax.Precision.HIGH
row_forms = ("kj,rjm->rkm", "rkm,ml->rkl")
column_forms = ("kj,jmc->kmc", "kmc,ml->klc")


def padded_2(cells, sides, width):
    for axis, dim in sides:
        count = lax.axis_size(axis)
        head = lax.slice_in_dim(cells, 0, width, axis=dim)
        tail = lax.slice_in_dim(cells, cells.shape[dim] - width, cells.shape[dim], axis=dim)
        cells = jnp.concatenate(
            [
                lax.ppermute(tail, axis, [(i, (i + 1) % count) for i in range(count)]),
                cells,
                lax.ppermute(head, axis, [((i + 1) % count, i) for i in range(count)]),
            ],
            axis=dim,
        )
    return cells


def split_length(length):
    factor = int(math.isqrt(length))
    while length % factor:
        factor -= 1
    return (length // factor, factor)


def dft_tables(length):
    positions = jnp.arange(length, dtype=jnp.int32)
    product = positions[:, None] * positions[None, :] % length
    angles = product.astype(jnp.float32) * (2.0 * math.pi / length)
    return (jnp.cos(angles), -jnp.sin(angles))


def prepare(length, twist_shape):
    outer_len, inner_len = split_length(length)
    cos_outer, sin_outer = dft_tables(outer_len)
    cos_inner, sin_inner = dft_tables(inner_len)
    outer_pos = jnp.arange(outer_len, dtype=jnp.int32)
    inner_pos = jnp.arange(inner_len, dtype=jnp.int32)
    product = outer_pos[:, None] * inner_pos[None, :] % length
    angles = product.astype(jnp.float32) * (2.0 * math.pi / length)
    twist_real = jnp.cos(angles).reshape(twist_shape)
    twist_imag = (-jnp.sin(angles)).reshape(twist_shape)
    return (
        outer_len,
        inner_len,
        cos_outer,
        sin_outer,
        cos_inner,
        sin_inner,
        twist_real,
        twist_imag,
    )


def contract(form, left, right):
    return jnp.einsum(
        form, left, right, precision=dft_precision, preferred_element_type=jnp.float32
    )


def forward(values, tables, forms):
    outer_len, inner_len, cos_outer, sin_outer, cos_inner, sin_inner, twist_real, twist_imag = (
        tables
    )
    first_real = contract(forms[0], cos_outer, values)
    first_imag = contract(forms[0], sin_outer, values)
    turned_real = first_real * twist_real - first_imag * twist_imag
    turned_imag = first_real * twist_imag + first_imag * twist_real
    out_real = contract(forms[1], turned_real, cos_inner) - contract(
        forms[1], turned_imag, sin_inner
    )
    out_imag = contract(forms[1], turned_real, sin_inner) + contract(
        forms[1], turned_imag, cos_inner
    )
    return (out_real, out_imag)


def inverse(spec_real, spec_imag, tables, forms):
    outer_len, inner_len, cos_outer, sin_outer, cos_inner, sin_inner, twist_real, twist_imag = (
        tables
    )
    back_real = contract(forms[1], spec_real, cos_inner) + contract(forms[1], spec_imag, sin_inner)
    back_imag = contract(forms[1], spec_imag, cos_inner) - contract(forms[1], spec_real, sin_inner)
    turned_real = back_real * twist_real + back_imag * twist_imag
    turned_imag = back_imag * twist_real - back_real * twist_imag
    result = contract(forms[0], cos_outer, turned_real) + contract(forms[0], sin_outer, turned_imag)
    return result / float(outer_len * inner_len)


def convolve(values, filter_spec, tables, forms):
    spec_real, spec_imag = forward(values, tables, forms)
    filter_real, filter_imag = filter_spec
    prod_real = spec_real * filter_real - spec_imag * filter_imag
    prod_imag = spec_real * filter_imag + spec_imag * filter_real
    return inverse(prod_real, prod_imag, tables, forms)


def body(pixels, row_taps, column_taps, stencil):
    rows_dev, row_length = pixels.shape
    devices_rows = lax.axis_size("rows")
    whole_row, whole_column = (
        lax.all_gather(row_taps, "rows", axis=0, tiled=True),
        lax.all_gather(column_taps, "rows", axis=0, tiled=True),
    )
    column_length = whole_column.shape[0]
    row_tables = prepare(row_length, (1, split_length(row_length)[0], split_length(row_length)[1]))
    column_tables = prepare(
        column_length, (split_length(column_length)[0], split_length(column_length)[1], 1)
    )
    row_filter = forward(whole_row.reshape(1, row_tables[0], row_tables[1]), row_tables, row_forms)
    column_filter = forward(
        whole_column.reshape(column_tables[0], column_tables[1], 1), column_tables, column_forms
    )
    cols_dev = row_length // devices_rows
    lane_width = min(128, cols_dev)
    groups = cols_dev // lane_width
    padded = padded_2(pixels, (("rows", 0),), 1)
    shaped = pixels.reshape(pixels.shape[0], row_tables[0], row_tables[1])
    blocks = (
        convolve(shaped, row_filter, row_tables, row_forms)
        .reshape(pixels.shape)
        .reshape(rows_dev, groups, devices_rows * lane_width)
    )
    moved = lax.all_to_all(blocks, "rows", split_axis=2, concat_axis=0, tiled=True)
    shaped = moved.reshape(column_tables[0], column_tables[1], -1)
    result = lax.all_to_all(
        convolve(shaped, column_filter, column_tables, column_forms).reshape(moved.shape),
        "rows",
        split_axis=0,
        concat_axis=2,
        tiled=True,
    )
    convolved = result.reshape(rows_dev, row_length)
    filtered = convolved
    for offset_row in range(3):
        row_band = padded[offset_row : offset_row + rows_dev]
        for offset_col in range(3):
            filtered = filtered + stencil[offset_row, offset_col] * jnp.roll(
                row_band, 1 - offset_col, axis=1
            )
    return filtered


def split_bf16(values):
    high = values.astype(jnp.bfloat16)
    low = (values - high.astype(jnp.float32)).astype(jnp.bfloat16)
    return high, low


def mm(left, right):
    return jnp.dot(left, right, preferred_element_type=jnp.float32)


def mm3(left, right):
    return mm(left[0], right[0]) + (mm(left[0], right[1]) + mm(left[1], right[0]))


def host_tables(side):
    length = side * side
    index = np.arange(side)
    product = index[:, None] * index[None, :]
    angle = 2.0 * np.pi * (product % side) / side
    cos, sin = np.cos(angle), np.sin(angle)
    table = np.block([[cos, sin], [-sin, cos]]).astype(np.float32)

    def halves(array):
        high = array.astype(jnp.bfloat16)
        low = (array - high.astype(np.float32)).astype(jnp.bfloat16)
        return high, low

    fwd_high, fwd_low = halves(table)
    inv_high, inv_low = halves(np.ascontiguousarray(table.T))
    turn = 2.0 * np.pi * product / length
    return (
        fwd_high,
        fwd_low,
        inv_high,
        inv_low,
        np.cos(turn).astype(np.float32),
        (-np.sin(turn)).astype(np.float32),
    )


def kernel(
    dims,
    pixels,
    row_taps,
    column_taps,
    stencil,
    tables_in,
    twists_in,
    out,
    padded,
    tables,
    twists,
    top_row,
    bottom_row,
    recv,
    recv_high,
    recv_low,
    ready,
    back,
    cells_by_row,
    halo_above,
    halo_below,
    all_row,
    all_column,
    circ_high,
    circ_low,
    filter_real,
    filter_imag,
    send_px,
    recv_px,
    send_row,
    recv_row,
    send_col,
    recv_col,
    send_halo,
    recv_halo,
    send_back,
    recv_back,
    send_last,
    recv_last,
    local_sem,
):
    count, rows_dev, side, pieces = dims
    groups = rows_dev // 8
    cols_dev = side * side // count
    a_dev = cols_dev // 128
    column_length = count * rows_dev
    piece_cols = cols_dev // pieces
    own = slice(8, 8 + rows_dev)
    me = lax.axis_index("rows")

    def peer(step):
        return lax.rem(me + step, count)

    def source(step):
        return lax.rem(me + count - step, count)

    load_px = pltpu.make_async_copy(pixels, padded.at[own, :], local_sem.at[0])
    load_tables = pltpu.make_async_copy(tables_in, tables, local_sem.at[1])
    load_twists = pltpu.make_async_copy(twists_in, twists, local_sem.at[2])
    load_px.start()
    load_tables.start()
    load_twists.start()

    barrier = pltpu.get_barrier_semaphore()

    @pl.loop(1, count)
    def _(step):
        pl.semaphore_signal(barrier, inc=1, device_id={"rows": peer(step)})

    pl.semaphore_wait(barrier, count - 1)

    def columns_of(rank, piece):
        return pl.ds(pl.multiple_of(rank * cols_dev + piece * piece_cols, 128), piece_cols)

    def rows_of(rank):
        return pl.ds(pl.multiple_of(rank * rows_dev, 16), rows_dev)

    def px_copy(piece, step):
        to = peer(step)
        return pltpu.make_async_remote_copy(
            src_ref=padded.at[own, columns_of(to, piece)],
            dst_ref=recv.at[piece, rows_of(me), :],
            send_sem=send_px.at[piece, step],
            recv_sem=recv_px.at[piece, step],
            device_id={"rows": to},
        )

    def row_copy(step):
        return pltpu.make_async_remote_copy(
            src_ref=row_taps,
            dst_ref=all_row.at[me],
            send_sem=send_row.at[step],
            recv_sem=recv_row.at[step],
            device_id={"rows": peer(step)},
        )

    def col_copy(step):
        return pltpu.make_async_remote_copy(
            src_ref=column_taps,
            dst_ref=all_column.at[me],
            send_sem=send_col.at[step],
            recv_sem=recv_col.at[step],
            device_id={"rows": peer(step)},
        )

    def halo_copy(which):
        return pltpu.make_async_remote_copy(
            src_ref=(bottom_row, top_row)[which],
            dst_ref=(halo_above, halo_below)[which],
            send_sem=send_halo.at[which],
            recv_sem=recv_halo.at[which],
            device_id={"rows": peer(1 if which == 0 else count - 1)},
        )

    load_px.wait()

    @pl.loop(1, count)
    def _(step):
        px_copy(0, step).start()
        col_copy(step).start()

    top_row[...] = padded[8:9, :]
    bottom_row[...] = padded[7 + rows_dev : 8 + rows_dev, :]
    halo_copy(0).start()
    halo_copy(1).start()

    @pl.loop(1, count)
    def _(step):
        row_copy(step).start()

    for piece in range(1, pieces):

        @pl.loop(1, count)
        def _(step, piece=piece):
            px_copy(piece, step).start()

    all_row[me] = row_taps[...]
    all_column[me] = column_taps[...]
    load_tables.wait()
    load_twists.wait()

    @pl.loop(1, count)
    def _(step):
        col_copy(step).wait_recv()

    per_block = 128 // rows_dev
    lines = []
    for block in reversed(range(column_length // 128)):
        total = all_column[block * per_block]
        for rank in range(block * per_block + 1, (block + 1) * per_block):
            total = total + all_column[rank]
        lines.append(total)
    line = jnp.concatenate(lines, axis=1)
    line = jnp.broadcast_to(line, (128, column_length))
    turned = [
        pltpu.roll(line, block * 128 + 1, 1, stride=1, stride_axis=0)
        for block in range(column_length // 128)
    ]
    for group in range(groups):
        part = jnp.concatenate(
            [
                turned[rank // per_block][
                    (rank % per_block) * rows_dev + group * 8 :
                    (rank % per_block) * rows_dev + group * 8 + 8
                ]
                for rank in range(count)
            ],
            axis=0,
        )
        high, low = split_bf16(part)
        circ_high[group] = high
        circ_low[group] = low

    forward_table = (0, 1)
    inverse_table = (2, 3)

    def loaded(table):
        return (tables[table[0]], tables[table[1]])

    def swap(real, imag):
        return jnp.concatenate(
            [
                jnp.concatenate([real[:, :side], imag[:, :side]], axis=1),
                jnp.concatenate([real[:, side:], imag[:, side:]], axis=1),
            ],
            axis=0,
        )

    def spectrum(cells):
        first = mm3(loaded(forward_table), split_bf16(cells))
        real, imag = first[:side], first[side:]
        turn_r = jnp.concatenate([twists[0]] * 2, axis=1)
        turn_i = jnp.concatenate([twists[1]] * 2, axis=1)
        turned_cells = swap(real * turn_r - imag * turn_i, real * turn_i + imag * turn_r)
        return mm3(split_bf16(turned_cells), loaded(inverse_table))

    def inverse_of(real, imag):
        cells = jnp.concatenate([real, imag], axis=1)
        first = mm3(split_bf16(cells), loaded(forward_table))
        real, imag = first[:, :side], first[:, side:]
        turn_r = jnp.concatenate([twists[0]] * 2, axis=0)
        turn_i = jnp.concatenate([twists[1]] * 2, axis=0)
        back_real = real * turn_r + imag * turn_i
        back_imag = imag * turn_r - real * turn_i
        cells = jnp.concatenate(
            [
                jnp.concatenate([back_real[:side], back_real[side:]], axis=1),
                jnp.concatenate([back_imag[:side], back_imag[side:]], axis=1),
            ],
            axis=0,
        )
        return mm3(loaded(inverse_table), split_bf16(cells))

    def filter_spectrum():
        @pl.loop(1, count)
        def _(step):
            row_copy(step).wait_recv()

        row_filter = jnp.concatenate([all_row[rank] for rank in range(count)], axis=0)
        nothing = jnp.zeros_like(row_filter)
        filter_spec = spectrum(
            jnp.concatenate(
                [
                    jnp.concatenate([row_filter, nothing], axis=1),
                    jnp.concatenate([nothing, nothing], axis=1),
                ],
                axis=0,
            )
        )[:side]
        filter_real[...] = filter_spec[:, :side] * (1.0 / (side * side))
        filter_imag[...] = filter_spec[:, side:] * (1.0 / (side * side))

    def add_stencil():
        halo_copy(0).wait_recv()
        halo_copy(1).wait_recv()
        padded[7:8, :] = halo_above[...]
        padded[8 + rows_dev : 9 + rows_dev, :] = halo_below[...]
        width = side * side
        for group in range(groups):
            base = group * 8
            above = padded[7 + base : 15 + base, :]
            here = padded[8 + base : 16 + base, :]
            below = padded[9 + base : 17 + base, :]
            sums = [
                stencil[0, b] * above + stencil[1, b] * here + stencil[2, b] * below
                for b in range(3)
            ]
            out[base : base + 8, :] = (
                sums[1] + pltpu.roll(sums[0], 1, 1) + pltpu.roll(sums[2], width - 1, 1)
            )

    def back_copy(piece, step):
        to = peer(step)
        return pltpu.make_async_remote_copy(
            src_ref=ready.at[piece, rows_of(to), :],
            dst_ref=back.at[:, columns_of(me, piece)],
            send_sem=send_back.at[piece, step],
            recv_sem=recv_back.at[piece, step],
            device_id={"rows": to},
        )

    last = pieces - 1

    def last_copy(group, step):
        to = peer(step)
        return pltpu.make_async_remote_copy(
            src_ref=ready.at[last, pl.ds(pl.multiple_of(to * rows_dev + group * 8, 8), 8), :],
            dst_ref=back.at[pl.ds(group * 8, 8), columns_of(me, last)],
            send_sem=send_last.at[group, step],
            recv_sem=recv_last.at[group, step],
            device_id={"rows": to},
        )

    def take(piece, rank, values):
        at = rows_of(rank)
        high, low = split_bf16(values)
        recv_high[piece, at, :] = high
        recv_low[piece, at, :] = low

    def filtered_rows(piece, group):
        return mm3(
            (circ_high[group], circ_low[group]), (recv_high[piece], recv_low[piece])
        )

    for piece in range(pieces):
        take(piece, me, padded[own, columns_of(me, piece)])

    for piece in range(pieces):

        @pl.loop(1, count)
        def _(step, piece=piece):
            px_copy(piece, step).wait_recv()
            take(piece, source(step), recv[piece, rows_of(source(step)), :])

        for group in range(groups):
            done = filtered_rows(piece, group)
            for rank in range(count):
                at = rank * rows_dev + group * 8
                ready[piece, at : at + 8, :] = done[rank * 8 : rank * 8 + 8]
            if piece == last:

                @pl.loop(1, count)
                def _(step, group=group):
                    last_copy(group, step).start()

        if piece != last:

            @pl.loop(1, count)
            def _(step, piece=piece):
                back_copy(piece, step).start()

        back[:, columns_of(me, piece)] = ready[piece, rows_of(me), :]
        if piece == 0:
            filter_spectrum()
            add_stencil()

    flat_cells = cells_by_row.reshape(rows_dev * side, side)
    for piece in range(last):

        @pl.loop(1, count)
        def _(step, piece=piece):
            back_copy(piece, step).wait_recv()

    for group in range(groups):

        @pl.loop(1, count)
        def _(step, group=group):
            last_copy(group, step).wait_recv()

        for a in range(side):
            flat_cells[pl.ds(group * 8 * side + a, 8, stride=side), :] = back[
                group * 8 : group * 8 + 8, a * side : (a + 1) * side
            ]
        for half in range(2):
            row = group * 8 + half * 4
            cells = jnp.concatenate(
                [
                    jnp.concatenate([cells_by_row[row], cells_by_row[row + 2]], axis=1),
                    jnp.concatenate([cells_by_row[row + 1], cells_by_row[row + 3]], axis=1),
                ],
                axis=0,
            )
            spec = spectrum(cells)
            real, imag = spec[:, :side], spec[:, side:]
            filt_r = jnp.concatenate([filter_real[...]] * 2, axis=0)
            filt_i = jnp.concatenate([filter_imag[...]] * 2, axis=0)
            done = inverse_of(real * filt_r - imag * filt_i, real * filt_i + imag * filt_r)
            cells_by_row[row] = done[:side, :side]
            cells_by_row[row + 1] = done[side:, :side]
            cells_by_row[row + 2] = done[:side, side:]
            cells_by_row[row + 3] = done[side:, side:]
        for a in range(side):
            cut = slice(a * side, (a + 1) * side)
            out[group * 8 : group * 8 + 8, cut] += flat_cells[
                pl.ds(group * 8 * side + a, 8, stride=side), :
            ]

    halo_copy(0).wait_send()
    halo_copy(1).wait_send()

    @pl.loop(1, count)
    def _(step):
        row_copy(step).wait_send()
        col_copy(step).wait_send()
        for piece in range(pieces):
            px_copy(piece, step).wait_send()
        for piece in range(last):
            back_copy(piece, step).wait_send()
        for group in range(groups):
            last_copy(group, step).wait_send()


def fits(pixels, row_taps, column_taps):
    rows_dev, row_length = pixels.shape
    count = lax.axis_size("rows")
    side = math.isqrt(row_length)
    return (
        side == 128
        and side * side == row_length
        and row_length % (count * 1024) == 0
        and rows_dev % 16 == 0
        and 128 % rows_dev == 0
        and (count * rows_dev) % 128 == 0
        and count % (128 // rows_dev) == 0
    )


def fused(pixels, row_taps, column_taps, stencil):
    rows_dev, row_length = pixels.shape
    count = lax.axis_size("rows")
    side = math.isqrt(row_length)
    column_length = rows_dev * count
    cols_dev = row_length // count
    a_dev = cols_dev // 128
    groups = rows_dev // 8
    me = lax.axis_index("rows")
    pieces = 4
    piece_cols = cols_dev // pieces
    per_block = 128 // rows_dev
    start = (per_block - 1 - me % per_block) * rows_dev
    wanted = start + rows_dev - 1 - jnp.arange(128, dtype=jnp.int32)
    held = jnp.arange(rows_dev, dtype=jnp.int32)
    placed = jnp.sum(
        jnp.where(wanted[:, None] == held[None, :], column_taps[None, :], 0.0), axis=1
    ).reshape(1, 128)
    made = host_tables(side)
    tables = jnp.asarray(np.stack(made[:4]))
    twists = jnp.asarray(np.stack(made[4:]))
    hbm = pl.BlockSpec(memory_space=pl.ANY)
    vmem = pl.BlockSpec(memory_space=pltpu.VMEM)
    f32, bf16 = jnp.float32, jnp.bfloat16
    dma = pltpu.SemaphoreType.DMA
    return pl.pallas_call(
        functools.partial(kernel, (count, rows_dev, side, pieces)),
        out_shape=jax.ShapeDtypeStruct(pixels.shape, f32),
        in_specs=[hbm, vmem, vmem, pl.BlockSpec(memory_space=pltpu.SMEM), hbm, hbm],
        out_specs=vmem,
        scratch_shapes=[
            pltpu.VMEM((rows_dev + 16, row_length), f32),
            pltpu.VMEM(tables.shape, bf16),
            pltpu.VMEM(twists.shape, f32),
            pltpu.VMEM((1, row_length), f32),
            pltpu.VMEM((1, row_length), f32),
            pltpu.VMEM((pieces, column_length, piece_cols), f32),
            pltpu.VMEM((pieces, column_length, piece_cols), bf16),
            pltpu.VMEM((pieces, column_length, piece_cols), bf16),
            pltpu.VMEM((pieces, column_length, piece_cols), f32),
            pltpu.VMEM((rows_dev, row_length), f32),
            pltpu.VMEM((rows_dev, side, side), f32),
            pltpu.VMEM((1, row_length), f32),
            pltpu.VMEM((1, row_length), f32),
            pltpu.VMEM((count, a_dev, 128), f32),
            pltpu.VMEM((count, 1, 128), f32),
            pltpu.VMEM((groups, count * 8, column_length), bf16),
            pltpu.VMEM((groups, count * 8, column_length), bf16),
            pltpu.VMEM((side, side), f32),
            pltpu.VMEM((side, side), f32),
            dma((pieces, count)),
            dma((pieces, count)),
            dma((count,)),
            dma((count,)),
            dma((count,)),
            dma((count,)),
            dma((2,)),
            dma((2,)),
            dma((pieces, count)),
            dma((pieces, count)),
            dma((groups, count)),
            dma((groups, count)),
            dma((3,)),
        ],
        compiler_params=pltpu.CompilerParams(
            collective_id=0, has_side_effects=True, vmem_limit_bytes=60 * 1024 * 1024
        ),
    )(pixels, row_taps.reshape(a_dev, 128), placed, stencil, tables, twists)


def chosen(pixels, row_taps, column_taps, stencil):
    if fits(pixels, row_taps, column_taps):
        return fused(pixels, row_taps, column_taps, stencil)
    return body(pixels, row_taps, column_taps, stencil)


def solution(mesh):
    in_specs = (
        P(("chan", "rows"), None),
        P(("chan", "rows")),
        P(("chan", "rows")),
        P("chan", None),
    )
    out_specs = P(("chan", "rows"), None)
    return jax.shard_map(chosen, mesh=mesh, in_specs=in_specs, out_specs=out_specs, check_vma=False)
```

```python
import functools
import math

import jax
import jax.numpy as jnp
import numpy as np
from jax import lax
from jax.experimental import pallas as pl
from jax.experimental.pallas import tpu as pltpu
from jax.sharding import PartitionSpec as P

dft_precision = lax.Precision.HIGH
row_forms = ("kj,rjm->rkm", "rkm,ml->rkl")
column_forms = ("kj,jmc->kmc", "kmc,ml->klc")


def padded_2(cells, sides, width):
    for axis, dim in sides:
        count = lax.axis_size(axis)
        head = lax.slice_in_dim(cells, 0, width, axis=dim)
        tail = lax.slice_in_dim(cells, cells.shape[dim] - width, cells.shape[dim], axis=dim)
        cells = jnp.concatenate(
            [
                lax.ppermute(tail, axis, [(i, (i + 1) % count) for i in range(count)]),
                cells,
                lax.ppermute(head, axis, [((i + 1) % count, i) for i in range(count)]),
            ],
            axis=dim,
        )
    return cells


def split_length(length):
    factor = int(math.isqrt(length))
    while length % factor:
        factor -= 1
    return (length // factor, factor)


def dft_tables(length):
    positions = jnp.arange(length, dtype=jnp.int32)
    product = positions[:, None] * positions[None, :] % length
    angles = product.astype(jnp.float32) * (2.0 * math.pi / length)
    return (jnp.cos(angles), -jnp.sin(angles))


def prepare(length, twist_shape):
    outer_len, inner_len = split_length(length)
    cos_outer, sin_outer = dft_tables(outer_len)
    cos_inner, sin_inner = dft_tables(inner_len)
    outer_pos = jnp.arange(outer_len, dtype=jnp.int32)
    inner_pos = jnp.arange(inner_len, dtype=jnp.int32)
    product = outer_pos[:, None] * inner_pos[None, :] % length
    angles = product.astype(jnp.float32) * (2.0 * math.pi / length)
    twist_real = jnp.cos(angles).reshape(twist_shape)
    twist_imag = (-jnp.sin(angles)).reshape(twist_shape)
    return (
        outer_len,
        inner_len,
        cos_outer,
        sin_outer,
        cos_inner,
        sin_inner,
        twist_real,
        twist_imag,
    )


def contract(form, left, right):
    return jnp.einsum(
        form, left, right, precision=dft_precision, preferred_element_type=jnp.float32
    )


def forward(values, tables, forms):
    outer_len, inner_len, cos_outer, sin_outer, cos_inner, sin_inner, twist_real, twist_imag = (
        tables
    )
    first_real = contract(forms[0], cos_outer, values)
    first_imag = contract(forms[0], sin_outer, values)
    turned_real = first_real * twist_real - first_imag * twist_imag
    turned_imag = first_real * twist_imag + first_imag * twist_real
    out_real = contract(forms[1], turned_real, cos_inner) - contract(
        forms[1], turned_imag, sin_inner
    )
    out_imag = contract(forms[1], turned_real, sin_inner) + contract(
        forms[1], turned_imag, cos_inner
    )
    return (out_real, out_imag)


def inverse(spec_real, spec_imag, tables, forms):
    outer_len, inner_len, cos_outer, sin_outer, cos_inner, sin_inner, twist_real, twist_imag = (
        tables
    )
    back_real = contract(forms[1], spec_real, cos_inner) + contract(forms[1], spec_imag, sin_inner)
    back_imag = contract(forms[1], spec_imag, cos_inner) - contract(forms[1], spec_real, sin_inner)
    turned_real = back_real * twist_real + back_imag * twist_imag
    turned_imag = back_imag * twist_real - back_real * twist_imag
    result = contract(forms[0], cos_outer, turned_real) + contract(forms[0], sin_outer, turned_imag)
    return result / float(outer_len * inner_len)


def convolve(values, filter_spec, tables, forms):
    spec_real, spec_imag = forward(values, tables, forms)
    filter_real, filter_imag = filter_spec
    prod_real = spec_real * filter_real - spec_imag * filter_imag
    prod_imag = spec_real * filter_imag + spec_imag * filter_real
    return inverse(prod_real, prod_imag, tables, forms)


def body(pixels, row_taps, column_taps, stencil):
    rows_dev, row_length = pixels.shape
    devices_rows = lax.axis_size("rows")
    whole_row, whole_column = (
        lax.all_gather(row_taps, "rows", axis=0, tiled=True),
        lax.all_gather(column_taps, "rows", axis=0, tiled=True),
    )
    column_length = whole_column.shape[0]
    row_tables = prepare(row_length, (1, split_length(row_length)[0], split_length(row_length)[1]))
    column_tables = prepare(
        column_length, (split_length(column_length)[0], split_length(column_length)[1], 1)
    )
    row_filter = forward(whole_row.reshape(1, row_tables[0], row_tables[1]), row_tables, row_forms)
    column_filter = forward(
        whole_column.reshape(column_tables[0], column_tables[1], 1), column_tables, column_forms
    )
    cols_dev = row_length // devices_rows
    lane_width = min(128, cols_dev)
    groups = cols_dev // lane_width
    padded = padded_2(pixels, (("rows", 0),), 1)
    shaped = pixels.reshape(pixels.shape[0], row_tables[0], row_tables[1])
    blocks = (
        convolve(shaped, row_filter, row_tables, row_forms)
        .reshape(pixels.shape)
        .reshape(rows_dev, groups, devices_rows * lane_width)
    )
    moved = lax.all_to_all(blocks, "rows", split_axis=2, concat_axis=0, tiled=True)
    shaped = moved.reshape(column_tables[0], column_tables[1], -1)
    result = lax.all_to_all(
        convolve(shaped, column_filter, column_tables, column_forms).reshape(moved.shape),
        "rows",
        split_axis=0,
        concat_axis=2,
        tiled=True,
    )
    convolved = result.reshape(rows_dev, row_length)
    filtered = convolved
    for offset_row in range(3):
        row_band = padded[offset_row : offset_row + rows_dev]
        for offset_col in range(3):
            filtered = filtered + stencil[offset_row, offset_col] * jnp.roll(
                row_band, 1 - offset_col, axis=1
            )
    return filtered


def split_bf16(values):
    high = values.astype(jnp.bfloat16)
    low = (values - high.astype(jnp.float32)).astype(jnp.bfloat16)
    return high, low


def mm(left, right):
    return jnp.dot(left, right, preferred_element_type=jnp.float32)


def mm3(left, right):
    return mm(left[0], right[0]) + (mm(left[0], right[1]) + mm(left[1], right[0]))


def host_tables(side):
    length = side * side
    index = np.arange(side)
    product = index[:, None] * index[None, :]
    angle = 2.0 * np.pi * (product % side) / side
    cos, sin = np.cos(angle), np.sin(angle)
    table = np.block([[cos, sin], [-sin, cos]]).astype(np.float32)

    def halves(array):
        high = array.astype(jnp.bfloat16)
        low = (array - high.astype(np.float32)).astype(jnp.bfloat16)
        return high, low

    fwd_high, fwd_low = halves(table)
    inv_high, inv_low = halves(np.ascontiguousarray(table.T))
    turn = 2.0 * np.pi * product / length
    return (
        fwd_high,
        fwd_low,
        inv_high,
        inv_low,
        np.cos(turn).astype(np.float32),
        (-np.sin(turn)).astype(np.float32),
    )


def kernel(
    dims,
    pixels,
    row_taps,
    column_taps,
    stencil,
    tables_in,
    twists_in,
    out,
    padded,
    tables,
    twists,
    top_row,
    bottom_row,
    recv,
    recv_high,
    recv_low,
    ready,
    back,
    cells_by_row,
    halo_above,
    halo_below,
    all_row,
    all_column,
    circ_high,
    circ_low,
    filter_real,
    filter_imag,
    send_px,
    recv_px,
    send_row,
    recv_row,
    send_col,
    recv_col,
    send_halo,
    recv_halo,
    send_back,
    recv_back,
    send_last,
    recv_last,
    local_sem,
):
    count, rows_dev, side, pieces = dims
    groups = rows_dev // 8
    cols_dev = side * side // count
    a_dev = cols_dev // 128
    column_length = count * rows_dev
    piece_cols = cols_dev // pieces
    own = slice(8, 8 + rows_dev)
    me = lax.axis_index("rows")

    planes = count // 4
    plane, core = me // 4, lax.rem(me, 2)
    way = jnp.where(plane < planes // 2, 1, planes - 1)

    def near(step):
        return plane * 4 + lax.rem(me + step, 4)

    def far(step):
        hop, turn = step % (planes - 1) + 1, step // (planes - 1)
        hop = lax.rem(hop + core * 1 - 1, planes - 1) + 1
        return lax.rem(plane + way * hop, planes) * 4 + lax.rem(me + turn, 4)

    def to_all(start):
        @pl.loop(1, 4)
        def _(step):
            start(near(step))

        @pl.loop(0, count - 4)
        def _(step):
            start(far(step))

    def peer(step):
        return lax.rem(me + step, count)

    load_px = pltpu.make_async_copy(pixels, padded.at[own, :], local_sem.at[0])
    load_tables = pltpu.make_async_copy(tables_in, tables, local_sem.at[1])
    load_twists = pltpu.make_async_copy(twists_in, twists, local_sem.at[2])
    load_px.start()
    load_tables.start()
    load_twists.start()

    barrier = pltpu.get_barrier_semaphore()

    @pl.loop(1, count)
    def _(step):
        pl.semaphore_signal(barrier, inc=1, device_id={"rows": peer(step)})

    pl.semaphore_wait(barrier, count - 1)

    def columns_of(rank, piece):
        return pl.ds(pl.multiple_of(rank * cols_dev + piece * piece_cols, 128), piece_cols)

    def rows_of(rank):
        return pl.ds(pl.multiple_of(rank * rows_dev, 16), rows_dev)

    def px_copy(piece, to, source):
        return pltpu.make_async_remote_copy(
            src_ref=padded.at[own, columns_of(to, piece)],
            dst_ref=recv.at[piece, rows_of(me), :],
            send_sem=send_px.at[piece, to],
            recv_sem=recv_px.at[piece, source],
            device_id={"rows": to},
        )

    def row_copy(to, source):
        return pltpu.make_async_remote_copy(
            src_ref=row_taps,
            dst_ref=all_row.at[me],
            send_sem=send_row.at[to],
            recv_sem=recv_row.at[source],
            device_id={"rows": to},
        )

    def col_copy(to, source):
        return pltpu.make_async_remote_copy(
            src_ref=column_taps,
            dst_ref=all_column.at[me],
            send_sem=send_col.at[to],
            recv_sem=recv_col.at[source],
            device_id={"rows": to},
        )

    def halo_copy(which):
        return pltpu.make_async_remote_copy(
            src_ref=(bottom_row, top_row)[which],
            dst_ref=(halo_above, halo_below)[which],
            send_sem=send_halo.at[which],
            recv_sem=recv_halo.at[which],
            device_id={"rows": peer(1 if which == 0 else count - 1)},
        )

    load_px.wait()

    def first_out(to):
        px_copy(0, to, me).start()
        col_copy(to, me).start()

    to_all(first_out)

    top_row[...] = padded[8:9, :]
    bottom_row[...] = padded[7 + rows_dev : 8 + rows_dev, :]
    halo_copy(0).start()
    halo_copy(1).start()

    to_all(lambda to: row_copy(to, me).start())

    for piece in range(1, pieces):
        to_all(lambda to, piece=piece: px_copy(piece, to, me).start())

    all_row[me] = row_taps[...]
    all_column[me] = column_taps[...]
    load_tables.wait()
    load_twists.wait()

    @pl.loop(1, count)
    def _(step):
        col_copy(peer(step), peer(step)).wait_recv()

    per_block = 128 // rows_dev
    lines = []
    for block in reversed(range(column_length // 128)):
        total = all_column[block * per_block]
        for rank in range(block * per_block + 1, (block + 1) * per_block):
            total = total + all_column[rank]
        lines.append(total)
    line = jnp.concatenate(lines, axis=1)
    line = jnp.broadcast_to(line, (128, column_length))
    turned = [
        pltpu.roll(line, block * 128 + 1, 1, stride=1, stride_axis=0)
        for block in range(column_length // 128)
    ]
    for group in range(groups):
        part = jnp.concatenate(
            [
                turned[rank // per_block][
                    (rank % per_block) * rows_dev + group * 8 :
                    (rank % per_block) * rows_dev + group * 8 + 8
                ]
                for rank in range(count)
            ],
            axis=0,
        )
        high, low = split_bf16(part)
        circ_high[group] = high
        circ_low[group] = low

    forward_table = (0, 1)
    inverse_table = (2, 3)

    def loaded(table):
        return (tables[table[0]], tables[table[1]])

    def swap(real, imag):
        return jnp.concatenate(
            [
                jnp.concatenate([real[:, :side], imag[:, :side]], axis=1),
                jnp.concatenate([real[:, side:], imag[:, side:]], axis=1),
            ],
            axis=0,
        )

    def spectrum(cells):
        first = mm3(loaded(forward_table), split_bf16(cells))
        real, imag = first[:side], first[side:]
        turn_r = jnp.concatenate([twists[0]] * 2, axis=1)
        turn_i = jnp.concatenate([twists[1]] * 2, axis=1)
        turned_cells = swap(real * turn_r - imag * turn_i, real * turn_i + imag * turn_r)
        return mm3(split_bf16(turned_cells), loaded(inverse_table))

    def inverse_of(real, imag):
        cells = jnp.concatenate([real, imag], axis=1)
        first = mm3(split_bf16(cells), loaded(forward_table))
        real, imag = first[:, :side], first[:, side:]
        turn_r = jnp.concatenate([twists[0]] * 2, axis=0)
        turn_i = jnp.concatenate([twists[1]] * 2, axis=0)
        back_real = real * turn_r + imag * turn_i
        back_imag = imag * turn_r - real * turn_i
        cells = jnp.concatenate(
            [
                jnp.concatenate([back_real[:side], back_real[side:]], axis=1),
                jnp.concatenate([back_imag[:side], back_imag[side:]], axis=1),
            ],
            axis=0,
        )
        return mm3(loaded(inverse_table), split_bf16(cells))

    def filter_spectrum():
        @pl.loop(1, count)
        def _(step):
            row_copy(peer(step), peer(step)).wait_recv()

        row_filter = jnp.concatenate([all_row[rank] for rank in range(count)], axis=0)
        nothing = jnp.zeros_like(row_filter)
        filter_spec = spectrum(
            jnp.concatenate(
                [
                    jnp.concatenate([row_filter, nothing], axis=1),
                    jnp.concatenate([nothing, nothing], axis=1),
                ],
                axis=0,
            )
        )[:side]
        filter_real[...] = filter_spec[:, :side] * (1.0 / (side * side))
        filter_imag[...] = filter_spec[:, side:] * (1.0 / (side * side))

    def add_stencil():
        halo_copy(0).wait_recv()
        halo_copy(1).wait_recv()
        padded[7:8, :] = halo_above[...]
        padded[8 + rows_dev : 9 + rows_dev, :] = halo_below[...]
        width = side * side
        for group in range(groups):
            base = group * 8
            above = padded[7 + base : 15 + base, :]
            here = padded[8 + base : 16 + base, :]
            below = padded[9 + base : 17 + base, :]
            sums = [
                stencil[0, b] * above + stencil[1, b] * here + stencil[2, b] * below
                for b in range(3)
            ]
            out[base : base + 8, :] = (
                sums[1] + pltpu.roll(sums[0], 1, 1) + pltpu.roll(sums[2], width - 1, 1)
            )

    def back_copy(piece, to, source):
        return pltpu.make_async_remote_copy(
            src_ref=ready.at[piece, rows_of(to), :],
            dst_ref=back.at[:, columns_of(me, piece)],
            send_sem=send_back.at[piece, to],
            recv_sem=recv_back.at[piece, source],
            device_id={"rows": to},
        )

    last = pieces - 1

    def last_copy(group, to, source):
        return pltpu.make_async_remote_copy(
            src_ref=ready.at[last, pl.ds(pl.multiple_of(to * rows_dev + group * 8, 8), 8), :],
            dst_ref=back.at[pl.ds(group * 8, 8), columns_of(me, last)],
            send_sem=send_last.at[group, to],
            recv_sem=recv_last.at[group, source],
            device_id={"rows": to},
        )

    def take(piece, rank, values):
        at = rows_of(rank)
        high, low = split_bf16(values)
        recv_high[piece, at, :] = high
        recv_low[piece, at, :] = low

    def filtered_rows(piece, group):
        return mm3(
            (circ_high[group], circ_low[group]), (recv_high[piece], recv_low[piece])
        )

    for piece in range(pieces):
        take(piece, me, padded[own, columns_of(me, piece)])

    for piece in range(pieces):

        @pl.loop(1, count)
        def _(step, piece=piece):
            source = peer(step)
            px_copy(piece, source, source).wait_recv()
            take(piece, source, recv[piece, rows_of(source), :])

        for group in range(groups):
            done = filtered_rows(piece, group)
            for rank in range(count):
                at = rank * rows_dev + group * 8
                ready[piece, at : at + 8, :] = done[rank * 8 : rank * 8 + 8]
            if piece == last:
                to_all(lambda to, group=group: last_copy(group, to, me).start())

        if piece != last:
            to_all(lambda to, piece=piece: back_copy(piece, to, me).start())

        back[:, columns_of(me, piece)] = ready[piece, rows_of(me), :]
        if piece == 0:
            filter_spectrum()
            add_stencil()

    flat_cells = cells_by_row.reshape(rows_dev * side, side)
    for piece in range(last):

        @pl.loop(1, count)
        def _(step, piece=piece):
            back_copy(piece, peer(step), peer(step)).wait_recv()

    for group in range(groups):

        @pl.loop(1, count)
        def _(step, group=group):
            last_copy(group, peer(step), peer(step)).wait_recv()

        for a in range(side):
            flat_cells[pl.ds(group * 8 * side + a, 8, stride=side), :] = back[
                group * 8 : group * 8 + 8, a * side : (a + 1) * side
            ]
        for half in range(2):
            row = group * 8 + half * 4
            cells = jnp.concatenate(
                [
                    jnp.concatenate([cells_by_row[row], cells_by_row[row + 2]], axis=1),
                    jnp.concatenate([cells_by_row[row + 1], cells_by_row[row + 3]], axis=1),
                ],
                axis=0,
            )
            spec = spectrum(cells)
            real, imag = spec[:, :side], spec[:, side:]
            filt_r = jnp.concatenate([filter_real[...]] * 2, axis=0)
            filt_i = jnp.concatenate([filter_imag[...]] * 2, axis=0)
            done = inverse_of(real * filt_r - imag * filt_i, real * filt_i + imag * filt_r)
            cells_by_row[row] = done[:side, :side]
            cells_by_row[row + 1] = done[side:, :side]
            cells_by_row[row + 2] = done[:side, side:]
            cells_by_row[row + 3] = done[side:, side:]
        for a in range(side):
            cut = slice(a * side, (a + 1) * side)
            out[group * 8 : group * 8 + 8, cut] += flat_cells[
                pl.ds(group * 8 * side + a, 8, stride=side), :
            ]

    halo_copy(0).wait_send()
    halo_copy(1).wait_send()

    @pl.loop(1, count)
    def _(step):
        row_copy(peer(step), peer(step)).wait_send()
        col_copy(peer(step), peer(step)).wait_send()
        for piece in range(pieces):
            px_copy(piece, peer(step), peer(step)).wait_send()
        for piece in range(last):
            back_copy(piece, peer(step), peer(step)).wait_send()
        for group in range(groups):
            last_copy(group, peer(step), peer(step)).wait_send()


def fits(pixels, row_taps, column_taps):
    rows_dev, row_length = pixels.shape
    count = lax.axis_size("rows")
    side = math.isqrt(row_length)
    return (
        side == 128
        and side * side == row_length
        and row_length % (count * 1024) == 0
        and rows_dev % 16 == 0
        and 128 % rows_dev == 0
        and (count * rows_dev) % 128 == 0
        and count % (128 // rows_dev) == 0
        and count % 4 == 0
        and count > 8
    )


def fused(pixels, row_taps, column_taps, stencil):
    rows_dev, row_length = pixels.shape
    count = lax.axis_size("rows")
    side = math.isqrt(row_length)
    column_length = rows_dev * count
    cols_dev = row_length // count
    a_dev = cols_dev // 128
    groups = rows_dev // 8
    me = lax.axis_index("rows")
    pieces = 2
    piece_cols = cols_dev // pieces
    per_block = 128 // rows_dev
    start = (per_block - 1 - me % per_block) * rows_dev
    wanted = start + rows_dev - 1 - jnp.arange(128, dtype=jnp.int32)
    held = jnp.arange(rows_dev, dtype=jnp.int32)
    placed = jnp.sum(
        jnp.where(wanted[:, None] == held[None, :], column_taps[None, :], 0.0), axis=1
    ).reshape(1, 128)
    made = host_tables(side)
    tables = jnp.asarray(np.stack(made[:4]))
    twists = jnp.asarray(np.stack(made[4:]))
    hbm = pl.BlockSpec(memory_space=pl.ANY)
    vmem = pl.BlockSpec(memory_space=pltpu.VMEM)
    f32, bf16 = jnp.float32, jnp.bfloat16
    dma = pltpu.SemaphoreType.DMA
    return pl.pallas_call(
        functools.partial(kernel, (count, rows_dev, side, pieces)),
        out_shape=jax.ShapeDtypeStruct(pixels.shape, f32),
        in_specs=[hbm, vmem, vmem, pl.BlockSpec(memory_space=pltpu.SMEM), hbm, hbm],
        out_specs=vmem,
        scratch_shapes=[
            pltpu.VMEM((rows_dev + 16, row_length), f32),
            pltpu.VMEM(tables.shape, bf16),
            pltpu.VMEM(twists.shape, f32),
            pltpu.VMEM((1, row_length), f32),
            pltpu.VMEM((1, row_length), f32),
            pltpu.VMEM((pieces, column_length, piece_cols), f32),
            pltpu.VMEM((pieces, column_length, piece_cols), bf16),
            pltpu.VMEM((pieces, column_length, piece_cols), bf16),
            pltpu.VMEM((pieces, column_length, piece_cols), f32),
            pltpu.VMEM((rows_dev, row_length), f32),
            pltpu.VMEM((rows_dev, side, side), f32),
            pltpu.VMEM((1, row_length), f32),
            pltpu.VMEM((1, row_length), f32),
            pltpu.VMEM((count, a_dev, 128), f32),
            pltpu.VMEM((count, 1, 128), f32),
            pltpu.VMEM((groups, count * 8, column_length), bf16),
            pltpu.VMEM((groups, count * 8, column_length), bf16),
            pltpu.VMEM((side, side), f32),
            pltpu.VMEM((side, side), f32),
            dma((pieces, count)),
            dma((pieces, count)),
            dma((count,)),
            dma((count,)),
            dma((count,)),
            dma((count,)),
            dma((2,)),
            dma((2,)),
            dma((pieces, count)),
            dma((pieces, count)),
            dma((groups, count)),
            dma((groups, count)),
            dma((3,)),
        ],
        compiler_params=pltpu.CompilerParams(
            collective_id=0, has_side_effects=True, vmem_limit_bytes=60 * 1024 * 1024
        ),
    )(pixels, row_taps.reshape(a_dev, 128), placed, stencil, tables, twists)


def chosen(pixels, row_taps, column_taps, stencil):
    if fits(pixels, row_taps, column_taps):
        return fused(pixels, row_taps, column_taps, stencil)
    return body(pixels, row_taps, column_taps, stencil)


def solution(mesh):
    in_specs = (
        P(("chan", "rows"), None),
        P(("chan", "rows")),
        P(("chan", "rows")),
        P("chan", None),
    )
    out_specs = P(("chan", "rows"), None)
    return jax.shard_map(chosen, mesh=mesh, in_specs=in_specs, out_specs=out_specs, check_vma=False)
```
